32 devices in a mesh: seq: 4 (over y, core), tp: 8 (over z, x).
Axes of the slice: x: 2, y: 2, z: 4, core: 2. Of those that a mesh axis runs over, the one named last changes fastest.
Arguments:
- tokens: bfloat16 [2048, 4608], P(('seq', 'tp')), may hold values from -6 to 6
- norm_gain: float32 [4608], replicated, may hold values from 0.1 to 1.9
- query_weight: bfloat16 [4608, 4096], P(None, 'tp'), may hold values from -6 to 6
- key_matrix: bfloat16 [4608, 2048], P(None, 'tp'), may hold values from -0.09375 to 0.09375
- value_matrix: bfloat16 [4608, 2048], P(None, 'tp'), may hold values from -0.09375 to 0.09375
- output_grad: bfloat16 [2048, 4096], P('seq', 'tp'), may hold values from -3 to 3
Outputs:
- input_gradient: bfloat16 [2048, 4608], P(('seq', 'tp'))
The draws below stay inside these ranges and needn't reach their ends.
All inputs are finite; a program needn't handle non-finite values.
Results may differ from the reference program's by a relative error of at most 0.014.
The reference program's roundings to bfloat16 on the way (of `normed` and `grad_query`) count: a program that leaves them out, or rounds other values in their place, can miss the bound.
Values may be sent and summed in bfloat16 or wider, within the bound.
A program may use at most 64 MiB of HBM per device.

```python
import math
import jax
import jax.numpy as jnp
from jax import lax

MODEL_WIDTH = 4608
HQ = 32
KEY_VALUE_HEADS = 16
HEAD_SIZE = 128
TOK_DEV = 512
WINDOW = 640
TOKENS = 2048


def draw_query_weight(key, part):
    head_scale = jnp.exp(jax.random.uniform(jax.random.fold_in(key, 11), (HQ,), jnp.float32, math.log(3.0), math.log(12.0)))
    column_scale = jnp.repeat(head_scale, HEAD_SIZE)
    entries = jax.random.truncated_normal(jax.random.fold_in(key, 12), -4.0, 4.0, (MODEL_WIDTH, HQ * HEAD_SIZE), jnp.float32)
    return (entries * column_scale[None, :] / math.sqrt(MODEL_WIDTH)).astype(jnp.bfloat16)


def strengthened(values, stream_key, source, target, blocks, factor):
    def block_of(axis_at):
        return (jnp.arange(values.shape[axis_at]) // (values.shape[axis_at] // blocks)).reshape((-1,) + (1,) * (values.ndim - 1 - axis_at))

    near = jax.random.permutation(stream_key, blocks)[block_of(target)]
    far = (block_of(target) + blocks // 2) % blocks
    return jnp.where((block_of(source) == near) | (block_of(source) == far), factor * values, values)


def block_scale(own_key, extent, pieces, smallest, top_value):
    gain = 1.0
    for axis_at, shards_of in pieces:
        steps = jax.random.uniform(jax.random.fold_in(jax.random.fold_in(own_key, 6), axis_at), (shards_of,), jnp.float32, smallest / len(pieces), top_value / len(pieces))
        gain = gain * jnp.repeat(jnp.exp(steps), extent[axis_at] // shards_of).reshape((-1,) + (1,) * (len(extent) - 1 - axis_at))
    return gain


def gaussian(own_key, shape, width, reach, split=(), kind=jnp.bfloat16):
    values = jax.random.normal(own_key, shape, jnp.float32) * width
    if len(split) > 0:
        values = block_scale(own_key, shape, split, -0.22, 0.18) * values
    return jnp.clip(values, min=-reach, max=reach).astype(kind)


def bell_draw_with(own_key, shape, width, bound, shards, heavy, held_as=jnp.bfloat16):
    result = width * jax.random.normal(own_key, shape, jnp.float32)
    if shards:
        result = result * block_scale(own_key, shape, shards, -0.22, 0.18)
    return jnp.clip(strengthened(result, jax.random.fold_in(own_key, 3), *heavy), -bound, bound).astype(held_as)


def setup_inputs(seed: int = 0) -> dict:
    key_of = jax.random.split(jax.random.key(seed), 7)
    tokens = gaussian(key_of[0], (TOKENS, MODEL_WIDTH), 1.0, 6.0, ((0, 32),))
    norm_gain = jnp.clip(1.0 + 0.18 * jax.random.normal(key_of[1], (MODEL_WIDTH,), jnp.float32), 0.1, 1.9)
    query_weight = draw_query_weight(jax.random.fold_in(key_of[6], 71), 0)
    key_matrix = gaussian(key_of[3], (MODEL_WIDTH, KEY_VALUE_HEADS * HEAD_SIZE), MODEL_WIDTH ** -0.5, 0.09375, ((1, 8),))
    value_matrix = gaussian(key_of[4], (MODEL_WIDTH, KEY_VALUE_HEADS * HEAD_SIZE), MODEL_WIDTH ** -0.5, 0.09375, ((1, 8),))
    output_grad = bell_draw_with(key_of[5], (TOKENS, HQ * HEAD_SIZE), 0.5, 3.0, ((0, 4), (1, 8)), (1, 0, 8, 2.0))
    return dict(tokens=tokens, norm_gain=norm_gain, query_weight=query_weight, key_matrix=key_matrix, value_matrix=value_matrix, output_grad=output_grad)


SCALE = 1.0 / 12.0
CAP = 50.0
EPS = 1e-06

def block_grads(query_blk, grad_blk, key_blk, value_blk, query_pos, key_pos):
    row_count = query_blk.shape[0]
    key_span = key_blk.shape[0]
    kv_heads = key_blk.shape[1] // HEAD_SIZE
    groups = query_blk.shape[1] // key_blk.shape[1]
    query_four = query_blk.reshape(row_count, kv_heads, groups, HEAD_SIZE).astype(jnp.float32)
    grad_four = grad_blk.reshape(row_count, kv_heads, groups, HEAD_SIZE).astype(jnp.float32)
    key_three = key_blk.reshape(key_span, kv_heads, HEAD_SIZE).astype(jnp.float32)
    value_three = value_blk.reshape(key_span, kv_heads, HEAD_SIZE).astype(jnp.float32)
    raw = jnp.einsum('qkgd,skd->kgqs', query_four, key_three)
    bent = jnp.tanh(raw * SCALE / CAP)
    capped = CAP * bent
    valid = (key_pos[None, :] <= query_pos[:, None]) & (key_pos[None, :] > query_pos[:, None] - WINDOW) & (key_pos[None, :] >= 0)
    expo = jnp.where(valid, jnp.exp(capped), 0.0)
    probs = expo / lax.optimization_barrier(jnp.sum(expo, axis=-1, keepdims=True))
    d_probs = jnp.einsum('qkgd,skd->kgqs', grad_four, value_three)
    delta = lax.optimization_barrier(jnp.sum(probs * d_probs, axis=-1, keepdims=True))
    d_raw = (probs * (d_probs - delta) * (1.0 - bent * bent) * SCALE).astype(jnp.bfloat16).astype(jnp.float32)
    probs_low = probs.astype(jnp.bfloat16).astype(jnp.float32)
    grad_query = jnp.einsum('kgqs,skd->qkgd', d_raw, key_three).reshape(row_count, kv_heads * groups * HEAD_SIZE)
    grad_key = jnp.einsum('kgqs,qkgd->skd', d_raw, query_four).reshape(key_span, kv_heads * HEAD_SIZE)
    grad_value = jnp.einsum('kgqs,qkgd->skd', probs_low, grad_four).reshape(key_span, kv_heads * HEAD_SIZE)
    return (grad_query, grad_key, grad_value)

def reference(tokens, norm_gain, query_weight, key_matrix, value_matrix, output_grad):
    total_rows = tokens.shape[0]
    key_cols = key_matrix.shape[1]
    block_rows = min(512, TOK_DEV)
    key_span = WINDOW + block_rows
    float_values = tokens.astype(jnp.float32)
    reciprocal_root_mean = lax.rsqrt(lax.optimization_barrier(jnp.mean(float_values * float_values, axis=1, keepdims=True)) + EPS)
    normed = (float_values * reciprocal_root_mean * norm_gain).astype(jnp.bfloat16)
    query_all = jnp.dot(normed, query_weight, preferred_element_type=jnp.float32).astype(jnp.bfloat16)
    key_all = jnp.dot(normed, key_matrix, preferred_element_type=jnp.float32).astype(jnp.bfloat16)
    value_all = jnp.dot(normed, value_matrix, preferred_element_type=jnp.float32).astype(jnp.bfloat16)
    pad_key = jnp.concatenate([jnp.zeros((WINDOW, key_cols), jnp.bfloat16), key_all], axis=0)
    pad_value = jnp.concatenate([jnp.zeros((WINDOW, key_cols), jnp.bfloat16), value_all], axis=0)

    def step_fn(carry, index_block):
        acc_key, acc_value = carry
        first_row = index_block * block_rows
        query_blk = lax.dynamic_slice_in_dim(query_all, first_row, block_rows, 0)
        grad_blk = lax.dynamic_slice_in_dim(output_grad, first_row, block_rows, 0)
        key_blk = lax.dynamic_slice_in_dim(pad_key, first_row, key_span, 0)
        value_blk = lax.dynamic_slice_in_dim(pad_value, first_row, key_span, 0)
        query_pos = first_row + jnp.arange(block_rows, dtype=jnp.int32)
        key_pos = first_row - WINDOW + jnp.arange(key_span, dtype=jnp.int32)
        grad_query, grad_key, grad_value = block_grads(query_blk, grad_blk, key_blk, value_blk, query_pos, key_pos)
        acc_key = lax.dynamic_update_slice_in_dim(acc_key, lax.dynamic_slice_in_dim(acc_key, first_row, key_span, 0) + grad_key, first_row, 0)
        acc_value = lax.dynamic_update_slice_in_dim(acc_value, lax.dynamic_slice_in_dim(acc_value, first_row, key_span, 0) + grad_value, first_row, 0)
        return ((acc_key, acc_value), grad_query.astype(jnp.bfloat16))
    zeros_acc = jnp.zeros((total_rows + WINDOW, key_cols), jnp.float32)
    (acc_key, acc_value), grad_blocks = lax.scan(step_fn, (zeros_acc, zeros_acc), jnp.arange(total_rows // block_rows, dtype=jnp.int32))
    grad_query = grad_blocks.reshape(total_rows, query_weight.shape[1])
    grad_key = acc_key[WINDOW:].astype(jnp.bfloat16)
    grad_value = acc_value[WINDOW:].astype(jnp.bfloat16)
    dims = (((1,), (1,)), ((), ()))
    d_norm = lax.dot_general(grad_query, query_weight, dims, preferred_element_type=jnp.float32)
    d_norm = d_norm + lax.dot_general(grad_key, key_matrix, dims, preferred_element_type=jnp.float32)
    d_norm = d_norm + lax.dot_general(grad_value, value_matrix, dims, preferred_element_type=jnp.float32)
    upper_limit = d_norm * norm_gain
    normalized_input = float_values * reciprocal_root_mean
    input_gradient = reciprocal_root_mean * (upper_limit - normalized_input * lax.optimization_barrier(jnp.mean(upper_limit * normalized_input, axis=1, keepdims=True)))
    return input_gradient.astype(jnp.bfloat16)
```

```python
import functools

import jax
import jax.numpy as jnp
from jax import lax
from jax.experimental import pallas as pl
from jax.experimental.pallas import tpu as pltpu
from jax.sharding import PartitionSpec as P

HEAD_SIZE = 128
WINDOW = 640


SCALE = 1.0 / 12.0
CAP = 50.0
EPS = 1e-06
VMEM_BYTES = 60 * 1024 * 1024


def shifted(block, axis, distance):
    devices = range(lax.axis_size(axis))
    route = [(i - distance, i) for i in devices if i - distance in devices]
    return lax.ppermute(block, axis, route)


def ring_place(index, n):
    odd = index % 2
    return (1 - odd) * (index // 2) + odd * (n - 1 - index // 2)


def ring_device(place, n):
    place = (place + n) % n
    late = place // (n // 2)
    return (1 - late) * 2 * place + late * (2 * (n - 1 - place) + 1)


def chunks_of(direction, hop, last):
    return (direction, 1 - direction) if hop < last else (direction,)


def greet(neighbours):
    barrier = pltpu.get_barrier_semaphore()
    for neighbour in neighbours:
        pl.semaphore_signal(
            barrier, inc=1, device_id={"tp": neighbour}, device_id_type=pl.DeviceIdType.MESH
        )
    pl.semaphore_wait(barrier, 2)


def load_weights(weights, held, sems):
    copies = []
    start = 0
    for i, weight in enumerate(weights):
        cols = weight.shape[1]
        copies.append(
            pltpu.make_async_copy(weight, held.at[:, start : start + cols], sems.at[i])
        )
        start += cols
    for copy in copies:
        copy.start()
    return copies


def gather_kernel(
    n, tokens, gain, wq, wk, wv, out, gathered, held, normed, send_sems, recv_sems, load_sems
):
    rows, width = tokens.shape
    half = rows // 2
    last = n // 2
    cols = out.shape[1]
    tile = 256
    place = ring_place(lax.axis_index("tp"), n)
    ahead = (ring_device(place + 1, n), ring_device(place - 1, n))
    loads = load_weights((wq, wk, wv), held, load_sems)
    greet(ahead)

    def sender(direction, hop, chunk):
        step = -(hop - 1) if direction == 0 else hop - 1
        owner = ring_device(place + step, n)
        part = pl.ds(chunk * half, half)
        source = tokens.at[part] if hop == 1 else gathered.at[owner, part]
        return pltpu.make_async_remote_copy(
            src_ref=source,
            dst_ref=gathered.at[owner, part],
            send_sem=send_sems.at[direction, hop - 1, chunk],
            recv_sem=recv_sems.at[direction, hop - 1, chunk],
            device_id={"tp": ahead[direction]},
            device_id_type=pl.DeviceIdType.MESH,
        )

    def project(sources):
        for i, (block, _) in enumerate(sources):
            values = block[...].astype(jnp.float32)
            scale = lax.rsqrt(jnp.mean(values * values, axis=1, keepdims=True) + EPS)
            normed[i * rows : (i + 1) * rows] = (values * scale * gain[...]).astype(jnp.bfloat16)
        count = len(sources) * rows

        def column(j, carry):
            at = pl.ds(pl.multiple_of(j * tile, tile), tile)
            product = jnp.dot(
                normed[:count], held[:, at], preferred_element_type=jnp.float32
            ).astype(jnp.bfloat16)
            for i, (_, owner) in enumerate(sources):
                out[pl.ds(pl.multiple_of(owner * rows, rows), rows), at] = product[
                    i * rows : (i + 1) * rows
                ]
            return carry

        lax.fori_loop(0, cols // tile, column, 0)

    sends = []
    for position in range(2):
        for direction in range(2):
            order = chunks_of(direction, 1, last)
            if position < len(order):
                sends.append(sender(direction, 1, order[position]))
                sends[-1].start()
    for copy in loads:
        copy.wait()
    project([(tokens, lax.axis_index("tp"))])
    for hop in range(1, last + 1):
        for position in range(2):
            for direction in range(2):
                order = chunks_of(direction, hop, last)
                if position < len(order):
                    chunk = order[position]
                    sender(direction, hop, chunk).wait_recv()
                    if hop < last and chunk in chunks_of(direction, hop + 1, last):
                        sends.append(sender(direction, hop + 1, chunk))
                        sends[-1].start()
        owners = [ring_device(place - hop, n)]
        if hop < last:
            owners.append(ring_device(place + hop, n))
        project([(gathered.at[owner], owner) for owner in owners])
    for copy in sends:
        copy.wait_send()


def gather_project(tokens, norm_gain, weights):
    n = lax.axis_size("tp")
    rows, width = tokens.shape
    cols = sum(weight.shape[1] for weight in weights)
    vmem = pl.BlockSpec(memory_space=pltpu.VMEM)
    hbm = pl.BlockSpec(memory_space=pl.ANY)
    return pl.pallas_call(
        functools.partial(gather_kernel, n),
        out_shape=jax.ShapeDtypeStruct((n * rows, cols), jnp.bfloat16),
        in_specs=[vmem, vmem, hbm, hbm, hbm],
        out_specs=vmem,
        scratch_shapes=[
            pltpu.VMEM((n, rows, width), jnp.bfloat16),
            pltpu.VMEM((width, cols), jnp.bfloat16),
            pltpu.VMEM((2 * rows, width), jnp.bfloat16),
            pltpu.SemaphoreType.DMA((2, n // 2, 2)),
            pltpu.SemaphoreType.DMA((2, n // 2, 2)),
            pltpu.SemaphoreType.DMA((3,)),
        ],
        compiler_params=pltpu.CompilerParams(
            collective_id=0, has_side_effects=True, vmem_limit_bytes=VMEM_BYTES
        ),
        name="gather_project",
    )(tokens, norm_gain.reshape(1, width), *weights)


def scatter_kernel(
    n,
    grads,
    tokens,
    gain,
    wq,
    wk,
    wv,
    out,
    outgoing,
    incoming,
    held,
    picked,
    total,
    send_sems,
    recv_sems,
    load_sems,
):
    rows, width = tokens.shape
    half = rows // 2
    last = n // 2
    tile = 256
    place = ring_place(lax.axis_index("tp"), n)
    ahead = (ring_device(place + 1, n), ring_device(place - 1, n))
    loads = load_weights((wq, wk, wv), held, load_sems)
    greet(ahead)

    def sender(direction, hop, chunk):
        part = pl.ds(chunk * half, half)
        return pltpu.make_async_remote_copy(
            src_ref=outgoing.at[direction, hop - 1, part],
            dst_ref=incoming.at[direction, hop - 1, part],
            send_sem=send_sems.at[direction, hop - 1, chunk],
            recv_sem=recv_sems.at[direction, hop - 1, chunk],
            device_id={"tp": ahead[direction]},
            device_id_type=pl.DeviceIdType.MESH,
        )

    def partial_sums(owners):
        for i, owner in enumerate(owners):
            picked[i * rows : (i + 1) * rows] = grads[
                pl.ds(pl.multiple_of(owner * rows, rows), rows)
            ]
        count = len(owners) * rows

        def column(j, carry):
            at = pl.ds(pl.multiple_of(j * tile, tile), tile)
            total[:count, at] = lax.dot_general(
                picked[:count],
                held[at, :],
                (((1,), (1,)), ((), ())),
                preferred_element_type=jnp.float32,
            )
            return carry

        lax.fori_loop(0, width // tile, column, 0)

    for copy in loads:
        copy.wait()
    sends = []
    for hop in range(last, 0, -1):
        owners = [ring_device(place + hop, n)]
        if hop < last:
            owners.append(ring_device(place - hop, n))
        partial_sums(owners)
        for position in (1, 0):
            for direction in range(2):
                order = chunks_of(direction, hop, last)
                if position < len(order):
                    chunk = order[position]
                    base = direction * rows if hop < last else 0
                    part = slice(chunk * half, (chunk + 1) * half)
                    value = total[base + chunk * half : base + (chunk + 1) * half]
                    if hop < last and chunk in chunks_of(direction, hop + 1, last):
                        sender(direction, hop + 1, chunk).wait_recv()
                        value = value + incoming[direction, hop, part].astype(jnp.float32)
                    outgoing[direction, hop - 1, part] = value.astype(jnp.bfloat16)
                    sends.append(sender(direction, hop, chunk))
                    sends[-1].start()
    partial_sums([lax.axis_index("tp")])
    for chunk in (1, 0):
        part = slice(chunk * half, (chunk + 1) * half)
        value = total[part]
        for direction in range(2):
            if chunk in chunks_of(direction, 1, last):
                sender(direction, 1, chunk).wait_recv()
                value = value + incoming[direction, 0, part].astype(jnp.float32)
        values = tokens[part].astype(jnp.float32)
        scale = lax.rsqrt(jnp.mean(values * values, axis=1, keepdims=True) + EPS)
        upper = value * gain[...]
        unit = values * scale
        out[part] = (
            scale * (upper - unit * jnp.mean(upper * unit, axis=1, keepdims=True))
        ).astype(jnp.bfloat16)
    for copy in sends:
        copy.wait_send()


def scatter_grads(grads, tokens, norm_gain, weights):
    n = lax.axis_size("tp")
    rows, width = tokens.shape
    cols = grads.shape[1]
    vmem = pl.BlockSpec(memory_space=pltpu.VMEM)
    hbm = pl.BlockSpec(memory_space=pl.ANY)
    return pl.pallas_call(
        functools.partial(scatter_kernel, n),
        out_shape=jax.ShapeDtypeStruct((rows, width), jnp.bfloat16),
        in_specs=[vmem, vmem, vmem, hbm, hbm, hbm],
        out_specs=vmem,
        scratch_shapes=[
            pltpu.VMEM((2, n // 2, rows, width), jnp.bfloat16),
            pltpu.VMEM((2, n // 2, rows, width), jnp.bfloat16),
            pltpu.VMEM((width, cols), jnp.bfloat16),
            pltpu.VMEM((2 * rows, cols), jnp.bfloat16),
            pltpu.VMEM((2 * rows, width), jnp.float32),
            pltpu.SemaphoreType.DMA((2, n // 2, 2)),
            pltpu.SemaphoreType.DMA((2, n // 2, 2)),
            pltpu.SemaphoreType.DMA((3,)),
        ],
        compiler_params=pltpu.CompilerParams(
            collective_id=1, has_side_effects=True, vmem_limit_bytes=VMEM_BYTES
        ),
        name="scatter_grads",
    )(grads, tokens, norm_gain.reshape(1, width), *weights)


def block_grads(query_blk, grad_blk, key_blk, value_blk, query_pos, key_pos):
    row_count = query_blk.shape[0]
    key_span = key_blk.shape[0]
    kv_heads = key_blk.shape[1] // HEAD_SIZE
    groups = query_blk.shape[1] // key_blk.shape[1]
    query_four = query_blk.reshape(row_count, kv_heads, groups, HEAD_SIZE)
    grad_four = grad_blk.reshape(row_count, kv_heads, groups, HEAD_SIZE)
    key_three = key_blk.reshape(key_span, kv_heads, HEAD_SIZE)
    value_three = value_blk.reshape(key_span, kv_heads, HEAD_SIZE)
    raw = jnp.einsum("qkgd,skd->kgqs", query_four, key_three, preferred_element_type=jnp.float32)
    bent = jnp.tanh(raw * SCALE / CAP)
    capped = CAP * bent
    valid = (
        (key_pos[None, :] <= query_pos[:, None])
        & (key_pos[None, :] > query_pos[:, None] - WINDOW)
        & (key_pos[None, :] >= 0)
    )
    expo = jnp.where(valid, jnp.exp(capped), 0.0)
    probs = expo / jnp.sum(expo, axis=-1, keepdims=True)
    d_probs = jnp.einsum(
        "qkgd,skd->kgqs", grad_four, value_three, preferred_element_type=jnp.float32
    )
    delta = jnp.sum(probs * d_probs, axis=-1, keepdims=True)
    d_raw = (probs * (d_probs - delta) * (1.0 - bent * bent) * SCALE).astype(jnp.bfloat16)
    probs_low = probs.astype(jnp.bfloat16)
    grad_query = jnp.einsum(
        "kgqs,skd->qkgd", d_raw, key_three, preferred_element_type=jnp.float32
    ).reshape(row_count, kv_heads * groups * HEAD_SIZE)
    grad_key = jnp.einsum(
        "kgqs,qkgd->skd", d_raw, query_four, preferred_element_type=jnp.float32
    ).reshape(key_span, kv_heads * HEAD_SIZE)
    grad_value = jnp.einsum(
        "kgqs,qkgd->skd", probs_low, grad_four, preferred_element_type=jnp.float32
    ).reshape(key_span, kv_heads * HEAD_SIZE)
    return (grad_query, grad_key, grad_value)


def on_device(tokens, norm_gain, query_weight, key_matrix, value_matrix, output_grad):
    local_rows = output_grad.shape[0]
    query_cols = query_weight.shape[1]
    key_cols = key_matrix.shape[1]
    reach = WINDOW - local_rows
    weights = (query_weight, key_matrix, value_matrix)
    joined = gather_project(tokens, norm_gain, weights)
    query_own = joined[:, :query_cols]
    pair_own = joined[:, query_cols:]
    near_pair = shifted(pair_own, "seq", 1)
    far_pair = shifted(pair_own[local_rows - reach :], "seq", 2)
    pairs = jnp.concatenate([far_pair, near_pair, pair_own], axis=0)
    anchor = lax.axis_index("seq") * local_rows
    query_pos = anchor + jnp.arange(local_rows, dtype=jnp.int32)
    key_pos = anchor - WINDOW + jnp.arange(WINDOW + local_rows, dtype=jnp.int32)
    grad_query, grad_key, grad_value = block_grads(
        query_own, output_grad, pairs[:, :key_cols], pairs[:, key_cols:], query_pos, key_pos
    )
    grad_pair = jnp.concatenate([grad_key, grad_value], axis=1)
    far_back = shifted(grad_pair[:reach], "seq", -2)
    back = shifted(grad_pair[reach:WINDOW], "seq", -1)
    own = grad_pair[WINDOW:] + back
    own = own.at[local_rows - reach :].add(far_back)
    grads = jnp.concatenate([grad_query.astype(jnp.bfloat16), own.astype(jnp.bfloat16)], axis=1)
    return scatter_grads(grads, tokens, norm_gain, weights)


def solution(mesh):
    return jax.shard_map(
        on_device,
        mesh=mesh,
        in_specs=(
            P(("seq", "tp"), None),
            P(),
            P(None, "tp"),
            P(None, "tp"),
            P(None, "tp"),
            P("seq", "tp"),
        ),
        out_specs=P(("seq", "tp"), None),
        check_vma=False,
    )
```

```python
import functools
import types

import jax
import jax.numpy as jnp
from jax import lax
from jax.experimental import pallas as pl
from jax.experimental.pallas import tpu as pltpu
from jax.sharding import PartitionSpec as P

HEAD_SIZE = 128
WINDOW = 640


SCALE = 1.0 / 12.0
CAP = 50.0
EPS = 1e-06
VMEM_BYTES = 60 * 1024 * 1024
QUERY_ROWS = 128
TILE = 256


def ring_place(index, n):
    odd = index % 2
    return (1 - odd) * (index // 2) + odd * (n - 1 - index // 2)


def ring_device(place, n):
    place = (place + n) % n
    late = place // (n // 2)
    return (1 - late) * 2 * place + late * (2 * (n - 1 - place) + 1)


def chunks_of(direction, hop, last):
    return (direction, 1 - direction) if hop < last else (direction,)


def greet(neighbours):
    barrier = pltpu.get_barrier_semaphore()
    for neighbour in neighbours:
        pl.semaphore_signal(
            barrier, inc=1, device_id=neighbour, device_id_type=pl.DeviceIdType.MESH
        )
    pl.semaphore_wait(barrier, len(neighbours))


def remote(source, target, send_sem, recv_sem, device):
    return pltpu.make_async_remote_copy(
        src_ref=source,
        dst_ref=target,
        send_sem=send_sem,
        recv_sem=recv_sem,
        device_id=device,
        device_id_type=pl.DeviceIdType.MESH,
    )


def load_weights(weights, held, sems):
    copies = []
    start = 0
    for i, weight in enumerate(weights):
        cols = weight.shape[1]
        copies.append(
            pltpu.make_async_copy(weight, held.at[:, start : start + cols], sems.at[i])
        )
        start += cols
    for copy in copies:
        copy.start()
    return copies


def rows_at(index, count):
    return pl.ds(pl.multiple_of(index * count, count), count)


def gather_phase(n, ring, onward, tokens, gain, loads, s):
    rows, _ = tokens.shape
    local = n * rows
    half = rows // 2
    last = n // 2
    query_cols = s.query.shape[1]
    pair_cols = s.pairs.shape[1]
    me = lax.axis_index("tp")
    place = ring_place(me, n)
    sends = []
    halos = []

    def sender(direction, hop, chunk):
        step = -(hop - 1) if direction == 0 else hop - 1
        owner = ring_device(place + step, n)
        part = pl.ds(chunk * half, half)
        return remote(
            tokens.at[part] if hop == 1 else s.gathered.at[owner, part],
            s.gathered.at[owner, part],
            s.gather_send.at[direction, hop - 1, chunk],
            s.gather_recv.at[direction, hop - 1, chunk],
            ring[direction],
        )

    def project(sources):
        for i, (block, _) in enumerate(sources):
            values = block[...].astype(jnp.float32)
            scale = lax.rsqrt(jnp.mean(values * values, axis=1, keepdims=True) + EPS)
            s.normed[i * rows : (i + 1) * rows] = (values * scale * gain[...]).astype(jnp.bfloat16)
        count = len(sources) * rows

        def column(target, base, first):
            def write(j, carry):
                product = jnp.dot(
                    s.normed[:count],
                    s.held[:, pl.ds(pl.multiple_of(first + j * TILE, TILE), TILE)],
                    preferred_element_type=jnp.float32,
                ).astype(jnp.bfloat16)
                for i, (_, owner) in enumerate(sources):
                    at = pl.ds(pl.multiple_of(base + owner * rows, rows), rows)
                    target[at, rows_at(j, TILE)] = product[i * rows : (i + 1) * rows]
                return carry

            return write

        lax.fori_loop(0, pair_cols // TILE, column(s.pairs, 2 * local, query_cols), 0)
        for _, owner in sources:
            for back in range(2):
                source = pl.ds(pl.multiple_of(2 * local + owner * rows, rows), rows)
                target = pl.ds(pl.multiple_of((1 - back) * local + owner * rows, rows), rows)
                halos.append(
                    remote(
                        s.pairs.at[source],
                        s.pairs.at[target],
                        s.halo_send.at[back, len(halos) // 2],
                        s.halo_recv.at[back, len(halos) // 2],
                        onward[back],
                    )
                )
                halos[-1].start()
        lax.fori_loop(0, query_cols // TILE, column(s.query, 0, 0), 0)

    for position in range(2):
        for direction in range(2):
            order = chunks_of(direction, 1, last)
            if position < len(order):
                sends.append(sender(direction, 1, order[position]))
                sends[-1].start()
    for copy in loads:
        copy.wait()
    project([(tokens, me)])
    for hop in range(1, last + 1):
        for position in range(2):
            for direction in range(2):
                order = chunks_of(direction, hop, last)
                if position < len(order):
                    chunk = order[position]
                    sender(direction, hop, chunk).wait_recv()
                    if hop < last and chunk in chunks_of(direction, hop + 1, last):
                        sends.append(sender(direction, hop + 1, chunk))
                        sends[-1].start()
        owners = [ring_device(place - hop, n)]
        if hop < last:
            owners.append(ring_device(place + hop, n))
        project([(s.gathered.at[owner], owner) for owner in owners])
    for copy in halos:
        copy.wait_recv()
    return sends + halos


def dot(lhs, rhs, left, right):
    return lax.dot_general(
        lhs, rhs, (((left,), (right,)), ((), ())), preferred_element_type=jnp.float32
    )


def attention_phase(backward, output_grad, s):
    local, query_cols = s.query.shape
    key_cols = s.pairs.shape[1] // 2
    kv_heads = key_cols // HEAD_SIZE
    groups = query_cols // key_cols
    reach = WINDOW - local
    span = WINDOW + QUERY_ROWS
    start = 2 * local - WINDOW
    anchor = lax.axis_index("seq") * local
    shape = (span, groups * QUERY_ROWS)
    key_at = lax.broadcasted_iota(jnp.int32, shape, 0)
    gap = key_at - lax.broadcasted_iota(jnp.int32, shape, 1) % QUERY_ROWS
    s.band[...] = jnp.where((gap > 0) & (gap <= WINDOW), key_at, -1)
    s.sums[...] = jnp.zeros_like(s.sums)
    sends = []

    def halo(head, back):
        part = pl.ds(reach, local) if back == 0 else pl.ds(0, reach)
        return remote(
            s.leaving.at[head, part],
            s.arriving.at[head, part],
            s.back_send.at[head, back],
            s.back_recv.at[head, back],
            backward[back],
        )

    for head in range(kv_heads):
        key_lanes = slice(head * HEAD_SIZE, (head + 1) * HEAD_SIZE)
        value_lanes = slice(key_cols + head * HEAD_SIZE, key_cols + (head + 1) * HEAD_SIZE)
        heads = [
            slice((head * groups + g) * HEAD_SIZE, (head * groups + g + 1) * HEAD_SIZE)
            for g in range(groups)
        ]

        def block(i, carry):
            own = rows_at(i, QUERY_ROWS)
            seen = pl.ds(pl.multiple_of(start + i * QUERY_ROWS, QUERY_ROWS), span)
            query = jnp.concatenate([s.query[own, lanes] for lanes in heads], axis=0)
            grad = jnp.concatenate([output_grad[own, lanes] for lanes in heads], axis=0)
            key = s.pairs[seen, key_lanes]
            value = s.pairs[seen, value_lanes]
            bent = jnp.tanh(dot(key, query, 1, 1) * (SCALE / CAP))
            first = jnp.maximum(WINDOW - anchor - i * QUERY_ROWS, 0)
            expo = jnp.where(s.band[...] >= first, jnp.exp(CAP * bent), 0.0)
            probs = expo * (1.0 / jnp.sum(expo, axis=0, keepdims=True))
            d_probs = dot(value, grad, 1, 1)
            delta = jnp.sum(probs * d_probs, axis=0, keepdims=True)
            d_raw = (probs * (d_probs - delta) * (1.0 - bent * bent) * SCALE).astype(jnp.bfloat16)
            at = pl.ds(pl.multiple_of(i * QUERY_ROWS, QUERY_ROWS), span)
            s.sums[head, at, :HEAD_SIZE] += dot(d_raw, query, 1, 0)
            s.sums[head, at, HEAD_SIZE:] += dot(probs.astype(jnp.bfloat16), grad, 1, 0)
            grad_query = dot(d_raw, key, 0, 0).astype(jnp.bfloat16)
            for g, lanes in enumerate(heads):
                s.grads[own, lanes] = grad_query[g * QUERY_ROWS : (g + 1) * QUERY_ROWS]
            return carry

        lax.fori_loop(0, local // QUERY_ROWS, block, 0)
        s.leaving[head] = s.sums[head, :WINDOW].astype(jnp.bfloat16)
        for back in range(2):
            sends.append(halo(head, back))
            sends[-1].start()
    for head in range(kv_heads):
        for back in range(2):
            halo(head, back).wait_recv()
        s.sums[head, WINDOW:] += s.arriving[head, reach:].astype(jnp.float32)
        s.sums[head, WINDOW + local - reach :] += s.arriving[head, :reach].astype(jnp.float32)
        for side in range(2):
            lanes = slice(side * HEAD_SIZE, (side + 1) * HEAD_SIZE)
            column = query_cols + side * key_cols + head * HEAD_SIZE
            s.grads[:, column : column + HEAD_SIZE] = s.sums[head, WINDOW:, lanes].astype(
                jnp.bfloat16
            )
    return sends


def scatter_phase(n, ring, tokens, gain, out, s):
    rows, width = tokens.shape
    half = rows // 2
    last = n // 2
    me = lax.axis_index("tp")
    place = ring_place(me, n)

    def sender(direction, hop, chunk):
        part = pl.ds(chunk * half, half)
        return remote(
            s.outgoing.at[direction, hop - 1, part],
            s.incoming.at[direction, hop - 1, part],
            s.scatter_send.at[direction, hop - 1, chunk],
            s.scatter_recv.at[direction, hop - 1, chunk],
            ring[direction],
        )

    def partial_sums(owners):
        for i, owner in enumerate(owners):
            s.picked[i * rows : (i + 1) * rows] = s.grads[rows_at(owner, rows)]
        count = len(owners) * rows

        def column(j, carry):
            at = rows_at(j, TILE)
            s.total[:count, at] = dot(s.picked[:count], s.held[at, :], 1, 1)
            return carry

        lax.fori_loop(0, width // TILE, column, 0)

    sends = []
    for hop in range(last, 0, -1):
        owners = [ring_device(place + hop, n)]
        if hop < last:
            owners.append(ring_device(place - hop, n))
        partial_sums(owners)
        for position in (1, 0):
            for direction in range(2):
                order = chunks_of(direction, hop, last)
                if position < len(order):
                    chunk = order[position]
                    base = direction * rows if hop < last else 0
                    part = slice(chunk * half, (chunk + 1) * half)
                    value = s.total[base + chunk * half : base + (chunk + 1) * half]
                    if hop < last and chunk in chunks_of(direction, hop + 1, last):
                        sender(direction, hop + 1, chunk).wait_recv()
                        value = value + s.incoming[direction, hop, part].astype(jnp.float32)
                    s.outgoing[direction, hop - 1, part] = value.astype(jnp.bfloat16)
                    sends.append(sender(direction, hop, chunk))
                    sends[-1].start()
    partial_sums([me])
    for chunk in (1, 0):
        part = slice(chunk * half, (chunk + 1) * half)
        value = s.total[part]
        for direction in range(2):
            if chunk in chunks_of(direction, 1, last):
                sender(direction, 1, chunk).wait_recv()
                value = value + s.incoming[direction, 0, part].astype(jnp.float32)
        values = tokens[part].astype(jnp.float32)
        scale = lax.rsqrt(jnp.mean(values * values, axis=1, keepdims=True) + EPS)
        upper = value * gain[...]
        unit = values * scale
        out[part] = (
            scale * (upper - unit * jnp.mean(upper * unit, axis=1, keepdims=True))
        ).astype(jnp.bfloat16)
    return sends


def kernel(names, n, seqs, tokens, gain, output_grad, wq, wk, wv, out, *scratch):
    s = types.SimpleNamespace(**dict(zip(names, scratch)))
    loads = load_weights((wq, wk, wv), s.held, s.load_sems)
    place = ring_place(lax.axis_index("tp"), n)
    block = lax.axis_index("seq")
    ring = [{"tp": ring_device(place + step, n)} for step in (1, -1)]
    onward = [{"seq": (block + step) % seqs} for step in (1, 2)]
    backward = [{"seq": (block + seqs - step) % seqs} for step in (1, 2)]
    greet(ring + onward + backward)
    sends = gather_phase(n, ring, onward, tokens, gain, loads, s)
    sends += attention_phase(backward, output_grad, s)
    sends += scatter_phase(n, ring, tokens, gain, out, s)
    for copy in sends:
        copy.wait_send()


def on_device(tokens, norm_gain, query_weight, key_matrix, value_matrix, output_grad):
    n = lax.axis_size("tp")
    rows, width = tokens.shape
    local, query_cols = output_grad.shape
    key_cols = key_matrix.shape[1]
    cols = query_cols + 2 * key_cols
    kv_heads = key_cols // HEAD_SIZE
    groups = query_cols // key_cols
    low, full = jnp.bfloat16, jnp.float32
    hops = pltpu.SemaphoreType.DMA((2, n // 2, 2))
    blocks = pltpu.SemaphoreType.DMA((2, n))
    heads = pltpu.SemaphoreType.DMA((kv_heads, 2))
    scratch = dict(
        gathered=pltpu.VMEM((n, rows, width), low),
        held=pltpu.VMEM((width, cols), low),
        normed=pltpu.VMEM((2 * rows, width), low),
        query=pltpu.VMEM((local, query_cols), low),
        pairs=pltpu.VMEM((3 * local, 2 * key_cols), low),
        band=pltpu.VMEM((WINDOW + QUERY_ROWS, groups * QUERY_ROWS), jnp.int32),
        sums=pltpu.VMEM((kv_heads, WINDOW + local, 2 * HEAD_SIZE), full),
        leaving=pltpu.VMEM((kv_heads, WINDOW, 2 * HEAD_SIZE), low),
        arriving=pltpu.VMEM((kv_heads, WINDOW, 2 * HEAD_SIZE), low),
        grads=pltpu.VMEM((local, cols), low),
        outgoing=pltpu.VMEM((2, n // 2, rows, width), low),
        incoming=pltpu.VMEM((2, n // 2, rows, width), low),
        picked=pltpu.VMEM((2 * rows, cols), low),
        total=pltpu.VMEM((2 * rows, width), full),
        gather_send=hops,
        gather_recv=hops,
        halo_send=blocks,
        halo_recv=blocks,
        back_send=heads,
        back_recv=heads,
        scatter_send=hops,
        scatter_recv=hops,
        load_sems=pltpu.SemaphoreType.DMA((3,)),
    )
    vmem = pl.BlockSpec(memory_space=pltpu.VMEM)
    hbm = pl.BlockSpec(memory_space=pl.ANY)
    return pl.pallas_call(
        functools.partial(kernel, tuple(scratch), n, lax.axis_size("seq")),
        out_shape=jax.ShapeDtypeStruct((rows, width), low),
        in_specs=[vmem, vmem, vmem, hbm, hbm, hbm],
        out_specs=vmem,
        scratch_shapes=list(scratch.values()),
        compiler_params=pltpu.CompilerParams(
            collective_id=0, has_side_effects=True, vmem_limit_bytes=VMEM_BYTES
        ),
        name="attention_backward",
    )(tokens, norm_gain.reshape(1, width), output_grad, query_weight, key_matrix, value_matrix)


def solution(mesh):
    return jax.shard_map(
        on_device,
        mesh=mesh,
        in_specs=(
            P(("seq", "tp"), None),
            P(),
            P(None, "tp"),
            P(None, "tp"),
            P(None, "tp"),
            P("seq", "tp"),
        ),
        out_specs=P(("seq", "tp"), None),
        check_vma=False,
    )
```

```python
import functools
import types

import jax
import jax.numpy as jnp
from jax import lax
from jax.experimental import pallas as pl
from jax.experimental.pallas import tpu as pltpu
from jax.sharding import PartitionSpec as P

HEAD_SIZE = 128
WINDOW = 640


SCALE = 1.0 / 12.0
CAP = 50.0
EPS = 1e-06
VMEM_BYTES = 60 * 1024 * 1024
QUERY_ROWS = 128
TILE = 256


def ring_place(index, n):
    odd = index % 2
    return (1 - odd) * (index // 2) + odd * (n - 1 - index // 2)


def ring_device(place, n):
    place = (place + n) % n
    late = place // (n // 2)
    return (1 - late) * 2 * place + late * (2 * (n - 1 - place) + 1)


def chunks_of(direction, hop, last):
    return (direction, 1 - direction) if hop < last else (direction,)


def greet(neighbours):
    barrier = pltpu.get_barrier_semaphore()
    for neighbour in neighbours:
        pl.semaphore_signal(
            barrier, inc=1, device_id=neighbour, device_id_type=pl.DeviceIdType.MESH
        )
    pl.semaphore_wait(barrier, len(neighbours))


def remote(source, target, send_sem, recv_sem, device):
    return pltpu.make_async_remote_copy(
        src_ref=source,
        dst_ref=target,
        send_sem=send_sem,
        recv_sem=recv_sem,
        device_id=device,
        device_id_type=pl.DeviceIdType.MESH,
    )


def load_weights(weights, held, sems):
    copies = []
    start = 0
    for i, weight in enumerate(weights):
        cols = weight.shape[1]
        copies.append(
            pltpu.make_async_copy(weight, held.at[:, start : start + cols], sems.at[i])
        )
        start += cols
    for copy in copies:
        copy.start()
    return copies


def rows_at(index, count):
    return pl.ds(pl.multiple_of(index * count, count), count)


def gather_phase(n, ring, onward, tokens, gain, loads, s):
    rows, _ = tokens.shape
    local = n * rows
    half = rows // 2
    last = n // 2
    query_cols = s.query.shape[1]
    pair_cols = s.pairs.shape[1]
    me = lax.axis_index("tp")
    place = ring_place(me, n)
    sends = []
    halos = []

    def sender(direction, hop, chunk):
        step = -(hop - 1) if direction == 0 else hop - 1
        owner = ring_device(place + step, n)
        part = pl.ds(chunk * half, half)
        return remote(
            tokens.at[part] if hop == 1 else s.gathered.at[owner, part],
            s.gathered.at[owner, part],
            s.gather_send.at[direction, hop - 1, chunk],
            s.gather_recv.at[direction, hop - 1, chunk],
            ring[direction],
        )

    def project(sources):
        for i, (block, _) in enumerate(sources):
            values = block[...].astype(jnp.float32)
            scale = lax.rsqrt(jnp.mean(values * values, axis=1, keepdims=True) + EPS)
            s.normed[i * rows : (i + 1) * rows] = (values * scale * gain[...]).astype(jnp.bfloat16)
        count = len(sources) * rows

        def column(target, base, first):
            def write(j, carry):
                product = jnp.dot(
                    s.normed[:count],
                    s.held[:, pl.ds(pl.multiple_of(first + j * TILE, TILE), TILE)],
                    preferred_element_type=jnp.float32,
                ).astype(jnp.bfloat16)
                for i, (_, owner) in enumerate(sources):
                    at = pl.ds(pl.multiple_of(base + owner * rows, rows), rows)
                    target[at, rows_at(j, TILE)] = product[i * rows : (i + 1) * rows]
                return carry

            return write

        lax.fori_loop(0, pair_cols // TILE, column(s.pairs, 2 * local, query_cols), 0)
        for _, owner in sources:
            for back in range(2):
                source = pl.ds(pl.multiple_of(2 * local + owner * rows, rows), rows)
                target = pl.ds(pl.multiple_of((1 - back) * local + owner * rows, rows), rows)
                halos.append(
                    remote(
                        s.pairs.at[source],
                        s.pairs.at[target],
                        s.halo_send.at[back, len(halos) // 2],
                        s.halo_recv.at[back, len(halos) // 2],
                        onward[back],
                    )
                )
                halos[-1].start()
        lax.fori_loop(0, query_cols // TILE, column(s.query, 0, 0), 0)

    for position in range(2):
        for direction in range(2):
            order = chunks_of(direction, 1, last)
            if position < len(order):
                sends.append(sender(direction, 1, order[position]))
                sends[-1].start()
    for copy in loads:
        copy.wait()
    project([(tokens, me)])
    for hop in range(1, last + 1):
        for position in range(2):
            for direction in range(2):
                order = chunks_of(direction, hop, last)
                if position < len(order):
                    chunk = order[position]
                    sender(direction, hop, chunk).wait_recv()
                    if hop < last and chunk in chunks_of(direction, hop + 1, last):
                        sends.append(sender(direction, hop + 1, chunk))
                        sends[-1].start()
        owners = [ring_device(place - hop, n)]
        if hop < last:
            owners.append(ring_device(place + hop, n))
        project([(s.gathered.at[owner], owner) for owner in owners])
    for copy in halos:
        copy.wait_recv()
    return sends + halos


def dot(lhs, rhs, left, right):
    return lax.dot_general(
        lhs, rhs, (((left,), (right,)), ((), ())), preferred_element_type=jnp.float32
    )


def attention_phase(backward, output_grad, s, meanwhile):
    local, query_cols = s.query.shape
    key_cols = s.pairs.shape[1] // 2
    kv_heads = key_cols // HEAD_SIZE
    groups = query_cols // key_cols
    reach = WINDOW - local
    span = WINDOW + QUERY_ROWS
    start = 2 * local - WINDOW
    anchor = lax.axis_index("seq") * local
    shape = (span, groups * QUERY_ROWS)
    key_at = lax.broadcasted_iota(jnp.int32, shape, 0)
    gap = key_at - lax.broadcasted_iota(jnp.int32, shape, 1) % QUERY_ROWS
    s.band[...] = jnp.where((gap > 0) & (gap <= WINDOW), key_at, -1)
    s.sums[...] = jnp.zeros_like(s.sums)
    sends = []

    early = local // QUERY_ROWS - 1
    pieces = ((0, reach, 1), (reach, early * QUERY_ROWS, 0), (early * QUERY_ROWS, WINDOW, 0))

    def halo(head, piece):
        first, end, back = pieces[piece]
        part = pl.ds(first, end - first)
        return remote(
            s.leaving.at[head, part],
            s.arriving.at[head, part],
            s.back_send.at[head, piece],
            s.back_recv.at[head, piece],
            backward[back],
        )

    for head in range(kv_heads):
        key_lanes = slice(head * HEAD_SIZE, (head + 1) * HEAD_SIZE)
        value_lanes = slice(key_cols + head * HEAD_SIZE, key_cols + (head + 1) * HEAD_SIZE)
        heads = [
            slice((head * groups + g) * HEAD_SIZE, (head * groups + g + 1) * HEAD_SIZE)
            for g in range(groups)
        ]

        def block(i, carry):
            own = rows_at(i, QUERY_ROWS)
            seen = pl.ds(pl.multiple_of(start + i * QUERY_ROWS, QUERY_ROWS), span)
            query = jnp.concatenate([s.query[own, lanes] for lanes in heads], axis=0)
            grad = jnp.concatenate([output_grad[own, lanes] for lanes in heads], axis=0)
            key = s.pairs[seen, key_lanes]
            value = s.pairs[seen, value_lanes]
            bent = jnp.tanh(dot(key, query, 1, 1) * (SCALE / CAP))
            first = jnp.maximum(WINDOW - anchor - i * QUERY_ROWS, 0)
            expo = jnp.where(s.band[...] >= first, jnp.exp(CAP * bent), 0.0)
            probs = expo * (1.0 / jnp.sum(expo, axis=0, keepdims=True))
            d_probs = dot(value, grad, 1, 1)
            delta = jnp.sum(probs * d_probs, axis=0, keepdims=True)
            d_raw = (probs * (d_probs - delta) * (1.0 - bent * bent) * SCALE).astype(jnp.bfloat16)
            at = pl.ds(pl.multiple_of(i * QUERY_ROWS, QUERY_ROWS), span)
            s.sums[head, at, :HEAD_SIZE] += dot(d_raw, query, 1, 0)
            s.sums[head, at, HEAD_SIZE:] += dot(probs.astype(jnp.bfloat16), grad, 1, 0)
            grad_query = dot(d_raw, key, 0, 0).astype(jnp.bfloat16)
            for g, lanes in enumerate(heads):
                s.grads[own, lanes] = grad_query[g * QUERY_ROWS : (g + 1) * QUERY_ROWS]
            return carry

        for blocks, ready in (((0, early), (0, 1)), ((early, early + 1), (2,))):
            lax.fori_loop(*blocks, block, 0)
            for piece in ready:
                first, end, _ = pieces[piece]
                s.leaving[head, first:end] = s.sums[head, first:end].astype(jnp.bfloat16)
                sends.append(halo(head, piece))
                sends[-1].start()
    meanwhile()
    for head in range(kv_heads):
        for piece in range(len(pieces)):
            halo(head, piece).wait_recv()
        s.sums[head, WINDOW:] += s.arriving[head, reach:].astype(jnp.float32)
        s.sums[head, WINDOW + local - reach :] += s.arriving[head, :reach].astype(jnp.float32)
        for side in range(2):
            lanes = slice(side * HEAD_SIZE, (side + 1) * HEAD_SIZE)
            column = query_cols + side * key_cols + head * HEAD_SIZE
            s.grads[:, column : column + HEAD_SIZE] = s.sums[head, WINDOW:, lanes].astype(
                jnp.bfloat16
            )
    return sends


def farthest_query_sums(n, rows, s):
    query_cols = s.query.shape[1]
    place = ring_place(lax.axis_index("tp"), n)
    s.picked[:rows, :query_cols] = s.grads[
        rows_at(ring_device(place + n // 2, n), rows), :query_cols
    ]

    def column(j, carry):
        at = rows_at(j, TILE)
        s.total[:rows, at] = dot(s.picked[:rows, :query_cols], s.held[at, :query_cols], 1, 1)
        return carry

    lax.fori_loop(0, s.total.shape[1] // TILE, column, 0)


def scatter_phase(n, ring, tokens, gain, out, s):
    rows, width = tokens.shape
    half = rows // 2
    last = n // 2
    split = width // 2
    query_cols = s.query.shape[1]
    me = lax.axis_index("tp")
    place = ring_place(me, n)

    def sender(direction, hop, chunk):
        part = pl.ds(chunk * half, half)
        return remote(
            s.outgoing.at[direction, hop - 1, part],
            s.incoming.at[direction, hop - 1, part],
            s.scatter_send.at[direction, hop - 1, chunk],
            s.scatter_recv.at[direction, hop - 1, chunk],
            ring[direction],
        )

    def far_sender(direction, side):
        part = pl.ds(direction * half, half)
        lanes = pl.ds(side * split, split)
        return remote(
            s.outgoing.at[direction, last - 1, part, lanes],
            s.incoming.at[direction, last - 1, part, lanes],
            s.scatter_send.at[direction, last - 1, side],
            s.scatter_recv.at[direction, last - 1, side],
            ring[direction],
        )

    def partial_sums(owners):
        for i, owner in enumerate(owners):
            s.picked[i * rows : (i + 1) * rows] = s.grads[rows_at(owner, rows)]
        count = len(owners) * rows

        def column(j, carry):
            at = rows_at(j, TILE)
            s.total[:count, at] = dot(s.picked[:count], s.held[at, :], 1, 1)
            return carry

        lax.fori_loop(0, width // TILE, column, 0)

    def arrivals(direction, hop, chunk):
        if hop < last:
            sender(direction, hop, chunk).wait_recv()
        else:
            for side in range(2):
                far_sender(direction, side).wait_recv()

    sends = []
    s.picked[:rows] = s.grads[rows_at(ring_device(place + last, n), rows)]
    for side in range(2):

        def add_pairs(j, carry):
            at = rows_at(j, TILE)
            s.total[:rows, at] += dot(
                s.picked[:rows, query_cols:], s.held[at, query_cols:], 1, 1
            )
            return carry

        tiles = split // TILE
        lax.fori_loop(side * tiles, (side + 1) * tiles, add_pairs, 0)
        lanes = slice(side * split, (side + 1) * split)
        for direction in range(2):
            part = slice(direction * half, (direction + 1) * half)
            s.outgoing[direction, last - 1, part, lanes] = s.total[part, lanes].astype(jnp.bfloat16)
            sends.append(far_sender(direction, side))
            sends[-1].start()
    for hop in range(last - 1, 0, -1):
        partial_sums([ring_device(place + hop, n), ring_device(place - hop, n)])
        for position in (1, 0):
            for direction in range(2):
                order = chunks_of(direction, hop, last)
                if position < len(order):
                    chunk = order[position]
                    base = direction * rows
                    part = slice(chunk * half, (chunk + 1) * half)
                    value = s.total[base + chunk * half : base + (chunk + 1) * half]
                    if chunk in chunks_of(direction, hop + 1, last):
                        arrivals(direction, hop + 1, chunk)
                        value = value + s.incoming[direction, hop, part].astype(jnp.float32)
                    s.outgoing[direction, hop - 1, part] = value.astype(jnp.bfloat16)
                    sends.append(sender(direction, hop, chunk))
                    sends[-1].start()
    partial_sums([me])
    for chunk in (1, 0):
        part = slice(chunk * half, (chunk + 1) * half)
        value = s.total[part]
        for direction in range(2):
            if chunk in chunks_of(direction, 1, last):
                arrivals(direction, 1, chunk)
                value = value + s.incoming[direction, 0, part].astype(jnp.float32)
        values = tokens[part].astype(jnp.float32)
        scale = lax.rsqrt(jnp.mean(values * values, axis=1, keepdims=True) + EPS)
        upper = value * gain[...]
        unit = values * scale
        out[part] = (
            scale * (upper - unit * jnp.mean(upper * unit, axis=1, keepdims=True))
        ).astype(jnp.bfloat16)
    return sends


def kernel(names, n, seqs, tokens, gain_ref, output_grad, wq, wk, wv, out, *scratch):
    s = types.SimpleNamespace(**dict(zip(names, scratch)))
    gain = s.gain
    loads = load_weights((wq, wk, wv), s.held, s.load_sems)
    place = ring_place(lax.axis_index("tp"), n)
    block = lax.axis_index("seq")
    ring = [{"tp": ring_device(place + step, n)} for step in (1, -1)]
    onward = [{"seq": (block + step) % seqs} for step in (1, 2)]
    backward = [{"seq": (block + seqs - step) % seqs} for step in (1, 2)]
    gain[...] = gain_ref[...].reshape(gain.shape)
    greet(ring + onward + backward)
    sends = gather_phase(n, ring, onward, tokens, gain, loads, s)
    meanwhile = functools.partial(farthest_query_sums, n, tokens.shape[0], s)
    sends += attention_phase(backward, output_grad, s, meanwhile)
    sends += scatter_phase(n, ring, tokens, gain, out, s)
    for copy in sends:
        copy.wait_send()


def on_device(tokens, norm_gain, query_weight, key_matrix, value_matrix, output_grad):
    n = lax.axis_size("tp")
    rows, width = tokens.shape
    local, query_cols = output_grad.shape
    key_cols = key_matrix.shape[1]
    cols = query_cols + 2 * key_cols
    kv_heads = key_cols // HEAD_SIZE
    groups = query_cols // key_cols
    low, full = jnp.bfloat16, jnp.float32
    hops = pltpu.SemaphoreType.DMA((2, n // 2, 2))
    blocks = pltpu.SemaphoreType.DMA((2, n))
    heads = pltpu.SemaphoreType.DMA((kv_heads, 3))
    scratch = dict(
        gain=pltpu.VMEM((1, width), full),
        gathered=pltpu.VMEM((n, rows, width), low),
        held=pltpu.VMEM((width, cols), low),
        normed=pltpu.VMEM((2 * rows, width), low),
        query=pltpu.VMEM((local, query_cols), low),
        pairs=pltpu.VMEM((3 * local, 2 * key_cols), low),
        band=pltpu.VMEM((WINDOW + QUERY_ROWS, groups * QUERY_ROWS), jnp.int32),
        sums=pltpu.VMEM((kv_heads, WINDOW + local, 2 * HEAD_SIZE), full),
        leaving=pltpu.VMEM((kv_heads, WINDOW, 2 * HEAD_SIZE), low),
        arriving=pltpu.VMEM((kv_heads, WINDOW, 2 * HEAD_SIZE), low),
        grads=pltpu.VMEM((local, cols), low),
        outgoing=pltpu.VMEM((2, n // 2, rows, width), low),
        incoming=pltpu.VMEM((2, n // 2, rows, width), low),
        picked=pltpu.VMEM((2 * rows, cols), low),
        total=pltpu.VMEM((2 * rows, width), full),
        gather_send=hops,
        gather_recv=hops,
        halo_send=blocks,
        halo_recv=blocks,
        back_send=heads,
        back_recv=heads,
        scatter_send=hops,
        scatter_recv=hops,
        load_sems=pltpu.SemaphoreType.DMA((3,)),
    )
    vmem = pl.BlockSpec(memory_space=pltpu.VMEM)
    hbm = pl.BlockSpec(memory_space=pl.ANY)
    return pl.pallas_call(
        functools.partial(kernel, tuple(scratch), n, lax.axis_size("seq")),
        out_shape=jax.ShapeDtypeStruct((rows, width), low),
        in_specs=[vmem, vmem, vmem, hbm, hbm, hbm],
        out_specs=vmem,
        scratch_shapes=list(scratch.values()),
        compiler_params=pltpu.CompilerParams(
            collective_id=0, has_side_effects=True, vmem_limit_bytes=VMEM_BYTES
        ),
        name="attention_backward",
    )(tokens, norm_gain, output_grad, query_weight, key_matrix, value_matrix)


def solution(mesh):
    return jax.shard_map(
        on_device,
        mesh=mesh,
        in_specs=(
            P(("seq", "tp"), None),
            P(),
            P(None, "tp"),
            P(None, "tp"),
            P(None, "tp"),
            P("seq", "tp"),
        ),
        out_specs=P(("seq", "tp"), None),
        check_vma=False,
    )
```
